128 devices in a mesh: hst: 2 (over core), row: 4 (over x), col: 16 (over z, y).
Axes of the slice: x: 4, y: 4, z: 4, core: 2. Of those that a mesh axis runs over, the one named last changes fastest.
Arguments:
- tables: bfloat16 [1024, 1024, 128], P(('hst', 'row', 'col')), may hold values from -6 to 6
- indices: int32 [1024, 2048, 4], P(('hst', 'row', 'col')), may hold values from 0 to 1023
- lengths: int32 [1024, 2048], P(('hst', 'row', 'col')), may hold values from 1 to 4, as said below
- table_slot: int32 [1024], replicated, may hold values from 0 to 1023, each once
- dense_feature: bfloat16 [2048, 128], P(('hst', 'row', 'col')), may hold values from -48 to 48
- left_proj: bfloat16 [128, 1025], replicated, may hold values from -0.1875 to 0.1875
- right_proj: bfloat16 [128, 1025], replicated, may hold values from -0.1875 to 0.1875
Outputs:
- interaction: bfloat16 [2048, 16384], P(('hst', 'row', 'col'))
The draws below stay inside these ranges and needn't reach their ends.
Inputs may be any that keep to these rules, and one draw needn't show every extreme that they name: Each bag uses its first lengths ids; some bag holds 4 ids.
All inputs are finite; a program needn't handle non-finite values.
Results may differ from the reference program's by a relative error of at most 0.0063.
Values may be sent and summed in bfloat16 or wider, within the bound.
A program may use at most 64 MiB of HBM per device.

```python
import jax
import jax.numpy as jnp
from jax import lax

E = 128
K = 128
ROWS = 1024
BAG = 4
B_DEV = 16
TABLES = 1024
BATCH = 2048


def draw_lengths(key, part):
    keys_all = jax.random.split(jax.random.fold_in(key, 7), 3)
    ceiling = jax.random.randint(keys_all[0], (TABLES,), 1, BAG + 1)
    chosen = jax.random.randint(keys_all[1], (), 0, TABLES)
    table_ids = jnp.arange(TABLES, dtype=jnp.int32)
    ceiling = jnp.where(table_ids == chosen, BAG, ceiling)
    random_bits = jax.random.randint(keys_all[2], (TABLES, BATCH), 0, 1 << 20)
    result = 1 + random_bits % ceiling[:, None]
    sample_ids = jnp.arange(BATCH, dtype=jnp.int32)
    forced = (table_ids[:, None] == chosen) & (sample_ids[None, :] == 0)
    return jnp.where(forced, BAG, result).astype(jnp.int32)


def with_ends(values, rng, low, top_value):
    spot = [jax.random.randint(jax.random.fold_in(rng, axis), (), 0, length) for axis, length in enumerate(values.shape)]
    main_axis = values.shape.index(max(values.shape))
    beside = spot[:main_axis] + [(spot[main_axis] + 1) % values.shape[main_axis]] + spot[main_axis + 1:]
    return values.at[tuple(spot)].set(low).at[tuple(beside)].set(top_value)


def shard_levels(stream_key, shape, shards, low, top_value):
    level = 1.0
    for dim, shards_of in shards:
        draws = jax.random.uniform(jax.random.fold_in(jax.random.fold_in(stream_key, 6), dim), (shards_of,), jnp.float32, low / len(shards), top_value / len(shards))
        level = level * jnp.repeat(jnp.exp(draws), shape[dim] // shards_of).reshape((-1,) + (1,) * (len(shape) - 1 - dim))
    return level


def centred(rng, shape, scale, bound, cuts=(), kind=jnp.bfloat16):
    values = scale * jax.random.normal(rng, shape, jnp.float32)
    if cuts:
        values = values * shard_levels(rng, shape, cuts, -0.22, 0.18)
    return jnp.clip(values, -bound, bound).astype(kind)


def setup_inputs(seed: int = 0) -> dict:
    streams_of = jax.random.split(jax.random.key(seed), 8)
    tables = centred(streams_of[0], (TABLES, ROWS, E), 1.0, 6.0, ((0, 128),))
    indices = with_ends(jax.random.randint(streams_of[1], (TABLES, BATCH, BAG), 0, ROWS), jax.random.fold_in(streams_of[1], 1), 0, ROWS - 1).astype(jnp.int32)
    lengths = draw_lengths(jax.random.fold_in(streams_of[7], 71), 0)
    table_slot = jax.random.permutation(streams_of[3], TABLES).astype(jnp.int32)
    dense_feature = centred(streams_of[4], (BATCH, E), 8.0, 48.0, ((0, 128),))
    left_proj = centred(streams_of[5], (K, TABLES + 1), (TABLES + 1) ** -0.5, 0.1875)
    right_proj = centred(streams_of[6], (K, TABLES + 1), (TABLES + 1) ** -0.5, 0.1875)
    return dict(tables=tables, indices=indices, lengths=lengths, table_slot=table_slot, dense_feature=dense_feature, left_proj=left_proj, right_proj=right_proj)


def reference(tables, indices, lengths, table_slot, dense_feature, left_proj, right_proj):
    table_ids = jnp.arange(TABLES, dtype=jnp.int32)[:, None]

    def one_block(start):
        row_ids = lax.dynamic_slice_in_dim(indices, start, B_DEV, 1)
        bag_lens = lax.dynamic_slice_in_dim(lengths, start, B_DEV, 1)
        dense_rows = lax.dynamic_slice_in_dim(dense_feature, start, B_DEV, 0)
        summed = jnp.zeros((TABLES, B_DEV, E), jnp.float32)
        for position in range(BAG):
            fetched = tables[table_ids, row_ids[:, :, position]].astype(jnp.float32)
            summed = summed + jnp.where((position < bag_lens)[:, :, None], fetched, 0.0)
        pooled = summed.astype(jnp.bfloat16)
        features = jnp.concatenate([dense_rows[None], pooled[table_slot]], axis=0).astype(jnp.float32)
        left_side = jnp.einsum("kg,gbe->kbe", left_proj.astype(jnp.float32), features).astype(jnp.bfloat16)
        right_side = jnp.einsum("kg,gbe->kbe", right_proj.astype(jnp.float32), features).astype(jnp.bfloat16)
        products = jnp.einsum("kbe,lbe->bkl", left_side.astype(jnp.float32), right_side.astype(jnp.float32))
        return (products * (1.0 / E)).reshape(B_DEV, K * K).astype(jnp.bfloat16)

    starts = jnp.arange(BATCH // B_DEV, dtype=jnp.int32) * B_DEV
    return lax.map(one_block, starts).reshape(BATCH, K * K)
```

```python
import functools

import jax
import jax.numpy as jnp
import numpy as np
from jax import lax
from jax.experimental import pallas as pl
from jax.experimental.pallas import tpu as pltpu
from jax.sharding import PartitionSpec as P

AXES = ("hst", "row", "col")
MESH = pl.DeviceIdType.MESH
LINE = (0, 1, 2, 1)


def split_offset(offset):
    return offset // 64, offset // 16 % 4, offset // 4 % 4, offset % 4


def hops(offset):
    _, dx, dz, dy = split_offset(offset)
    return LINE[dx] + LINE[dz] + LINE[dy]


ORDER = [0] + sorted(range(1, 128), key=lambda offset: -hops(offset))


def place():
    col = lax.axis_index("col")
    return lax.axis_index("hst"), lax.axis_index("row"), col // 4, lax.rem(col, 4)


def partner(me, dh, dx, dz, dy):
    h, x, z, y = me
    return (
        lax.rem(h + dh, 2),
        lax.rem(x + dx, 4),
        lax.rem(z + dz, 4) * 4 + lax.rem(y + dy, 4),
    )


def greet(me, sem, offsets):
    for offset in offsets:
        pl.semaphore_signal(sem, 1, device_id=partner(me, *offset), device_id_type=MESH)


X_LINE = [(0, i, 0, 0) for i in (1, 2, 3)]
Z_LINE = [(0, 0, i, 0) for i in (1, 2, 3)]
Y_LINE = [(0, 0, 0, i) for i in (1, 2, 3)]
H_LINE = [(1, 0, 0, 0)]


def kernel(
    tables, ids, lens, slots, dense, left_t, right_t, steps, out,
    table_t, pooled, send, recv, proj, shifted, total, wide,
    send_sem, recv_sem, x_sem, y_sem, h_sem,
):
    me = place()
    h, x, z, y = me
    tab_dev, bag, samples = ids.shape
    rows = tables.shape[1]
    width = tables.shape[2]
    own = dense.shape[0]
    block = 256
    groups = recv_sem.shape[0]
    per_group = len(ORDER) // groups
    depth = per_group * tab_dev

    barrier = pltpu.get_barrier_semaphore()
    greet(me, barrier, X_LINE + Y_LINE + Z_LINE + H_LINE)

    for t in range(tab_dev):
        table_t[t] = tables[t].T

    iota = lax.broadcasted_iota(jnp.int32, (16, block), 0).astype(jnp.int16)

    def pool_block(blk, _):
        start = pl.multiple_of(blk * block, block)
        for t in range(tab_dev):
            length = lens[pl.ds(t, 1), pl.ds(start, block)]
            row_ids = []
            for j in range(bag):
                row = ids[t, pl.ds(j, 1), pl.ds(start, block)]
                row_ids.append(jnp.where(j < length, row, -1))
            weights = []
            for j in range(bag):
                weight = jnp.ones((1, block), jnp.float32)
                for other in range(j + 1, bag):
                    weight += (row_ids[other] == row_ids[j]).astype(jnp.float32)
                weights.append(jnp.broadcast_to(weight, (16, block)).astype(jnp.bfloat16))
            keys = [jnp.broadcast_to(row, (16, block)).astype(jnp.int16) for row in row_ids]
            result = jnp.zeros((width, block), jnp.float32)
            for chunk in range(rows // block):
                pieces = []
                for piece in range(block // 16):
                    here = iota + jnp.int16(chunk * block + piece * 16)
                    counts = jnp.zeros((16, block), jnp.bfloat16)
                    for j in reversed(range(bag)):
                        counts = jnp.where(keys[j] == here, weights[j], counts)
                    pieces.append(counts)
                result += jnp.dot(
                    table_t[t, :, pl.ds(chunk * block, block)],
                    jnp.concatenate(pieces, axis=0),
                    preferred_element_type=jnp.float32,
                )
            pooled[pl.ds(t, block, stride=tab_dev), :] = result.T
        for part in range(block // own):
            piece = pooled[pl.ds(part * own * tab_dev, own * tab_dev), :]
            send[blk * (block // own) + part] = piece.reshape(own, tab_dev, width).astype(jnp.bfloat16)
        return 0

    blocks = samples // block
    quarter = blocks // 4
    lax.fori_loop(0, quarter, pool_block, 0)
    pl.semaphore_wait(barrier, 10)
    greet(me, x_sem, X_LINE)
    lax.fori_loop(quarter, 2 * quarter, pool_block, 0)
    pl.semaphore_wait(x_sem, 3)
    greet(me, y_sem, Y_LINE)
    lax.fori_loop(2 * quarter, 3 * quarter, pool_block, 0)
    pl.semaphore_wait(y_sem, 3)
    greet(me, h_sem, H_LINE)
    lax.fori_loop(3 * quarter, blocks, pool_block, 0)
    pl.semaphore_wait(h_sem, 1)

    for step in range(1, len(ORDER)):
        to_h, to_x, to_c = partner(me, *split_offset(ORDER[step]))
        pltpu.make_async_remote_copy(
            src_ref=send.at[to_h * 64 + to_x * 16 + to_c],
            dst_ref=recv.at[:, pl.ds(step * tab_dev, tab_dev), :],
            send_sem=send_sem,
            recv_sem=recv_sem.at[step // per_group],
            device_id=(to_h, to_x, to_c),
            device_id_type=MESH,
        ).start()
    recv[:, 0:tab_dev, :] = send[h * 64 + x * 16 + z * 4 + y]

    kept = left_t.shape[1]
    from_h = lax.rem(h + 2 - steps[0:1, :], 2)
    from_x = lax.rem(x + 4 - steps[1:2, :], 4)
    from_z = lax.rem(z + 4 - steps[2:3, :], 4)
    from_y = lax.rem(y + 4 - steps[3:4, :], 4)
    slot_here = (from_h * 64 + from_x * 16 + from_z * 4 + from_y) * tab_dev + steps[4:5, :]
    slot_here = slot_here.astype(jnp.float32)
    count = slots.shape[1]
    slot_col = jnp.broadcast_to(slots[...].astype(jnp.float32), (8, count)).T[:, 0:1]
    selector = jnp.where(slot_col == slot_here, 1.0, 0.0).astype(jnp.bfloat16)
    firsts = []
    for side, source in enumerate((left_t, right_t)):
        shifted[0 : count + 1, :] = source[...].astype(jnp.float32)
        firsts.append(shifted[0:8, :].T[:, 0:1])
        moved = shifted[1 : count + 1, :].T.astype(jnp.bfloat16)
        proj[pl.ds(side * kept, kept), :] = jnp.dot(
            moved, selector, preferred_element_type=jnp.float32
        ).astype(jnp.bfloat16)
    first = jnp.concatenate(firsts, axis=0)
    for b in range(own):
        row = dense[b : b + 1, :].astype(jnp.float32)
        total[b // 2, :, pl.ds(b % 2 * width, width)] = first * row

    for group in range(groups):
        arrived = per_group - (1 if group == 0 else 0)
        area = send.at[pl.ds(0, arrived)]
        pltpu.make_async_copy(area, area, recv_sem.at[group]).wait()
        last = group == groups - 1
        part = proj[:, pl.ds(group * depth, depth)]
        for pair in range(own // 2):
            both = jnp.concatenate(
                [recv[2 * pair, pl.ds(group * depth, depth), :], recv[2 * pair + 1, pl.ds(group * depth, depth), :]],
                axis=1,
            )
            mixed = total[pair] + jnp.dot(part, both, preferred_element_type=jnp.float32)
            if not last:
                total[pair] = mixed
                continue
            mixed = mixed.astype(jnp.bfloat16)
            for side in range(2):
                left = mixed[:kept, side * width : (side + 1) * width]
                right = mixed[kept:, side * width : (side + 1) * width]
                product = lax.dot_general(
                    left, right, (((1,), (1,)), ((), ())), preferred_element_type=jnp.float32
                )
                wide[pl.ds(2 * pair + side, kept, stride=own), :] = product * (1.0 / width)
    for k in range(kept):
        out[:, pl.ds(k * kept, kept)] = wide[pl.ds(k * own, own), :].astype(jnp.bfloat16)
    area = send.at[pl.ds(0, len(ORDER) - 1)]
    pltpu.make_async_copy(area, area, send_sem).wait()


def shards(tables, indices, lengths, table_slot, dense_feature, left_proj, right_proj):
    tab_dev, samples, bag = indices.shape
    width = tables.shape[2]
    rows = tables.shape[1]
    own = dense_feature.shape[0]
    kept = left_proj.shape[0]
    count = table_slot.shape[0]
    devices = len(ORDER)
    table = np.zeros((8, devices * tab_dev), np.int32)
    for step, offset in enumerate(ORDER):
        for t in range(tab_dev):
            table[:5, step * tab_dev + t] = (*split_offset(offset), t)
    vmem = pl.BlockSpec(memory_space=pltpu.VMEM)
    return pl.pallas_call(
        kernel,
        out_shape=jax.ShapeDtypeStruct((own, kept * kept), jnp.bfloat16),
        in_specs=[vmem] * 8,
        out_specs=vmem,
        scratch_shapes=[
            pltpu.VMEM((tab_dev, width, rows), jnp.bfloat16),
            pltpu.VMEM((256 * tab_dev, width), jnp.float32),
            pltpu.VMEM((devices, own, tab_dev, width), jnp.bfloat16),
            pltpu.VMEM((own, devices * tab_dev, width), jnp.bfloat16),
            pltpu.VMEM((2 * kept, devices * tab_dev), jnp.bfloat16),
            pltpu.VMEM((count + 8, kept), jnp.float32),
            pltpu.VMEM((own // 2, 2 * kept, 2 * width), jnp.float32),
            pltpu.VMEM((kept * own, kept), jnp.float32),
            pltpu.SemaphoreType.DMA,
            pltpu.SemaphoreType.DMA((4,)),
            pltpu.SemaphoreType.REGULAR,
            pltpu.SemaphoreType.REGULAR,
            pltpu.SemaphoreType.REGULAR,
        ],
        compiler_params=pltpu.CompilerParams(
            collective_id=0, has_side_effects=True, vmem_limit_bytes=60 * 2**20
        ),
    )(
        tables,
        jnp.transpose(indices, (0, 2, 1)),
        lengths,
        table_slot.reshape(1, count),
        dense_feature,
        left_proj.T,
        right_proj.T,
        jnp.asarray(table),
    )


def solution(mesh):
    spread = P(AXES)
    return jax.shard_map(
        shards,
        mesh=mesh,
        in_specs=(spread, spread, spread, P(), spread, P(), P()),
        out_specs=spread,
        check_vma=False,
    )
```

```python
import functools

import jax
import jax.numpy as jnp
import numpy as np
from jax import lax
from jax.experimental import pallas as pl
from jax.experimental.pallas import tpu as pltpu
from jax.sharding import PartitionSpec as P

AXES = ("hst", "row", "col")
MESH = pl.DeviceIdType.MESH
LINE = (0, 1, 2, 1)


def split_offset(offset):
    return offset // 64, offset // 16 % 4, offset // 4 % 4, offset % 4


def hops(offset):
    _, dx, dz, dy = split_offset(offset)
    return LINE[dx] + LINE[dz] + LINE[dy]


def far_first(offsets):
    return sorted(offsets, key=lambda offset: -hops(offset))


PLANE = far_first(range(1, 16))
SLAB = far_first(range(16, 64))
OTHER = far_first(range(64, 128))
ORDER = [0] + PLANE + SLAB + OTHER


def place():
    col = lax.axis_index("col")
    return lax.axis_index("hst"), lax.axis_index("row"), col // 4, lax.rem(col, 4)


def partner(me, dh, dx, dz, dy):
    h, x, z, y = me
    return (
        lax.rem(h + dh, 2),
        lax.rem(x + dx, 4),
        lax.rem(z + dz, 4) * 4 + lax.rem(y + dy, 4),
    )


def greet(me, sem, offsets):
    for offset in offsets:
        pl.semaphore_signal(sem, 1, device_id=partner(me, *offset), device_id_type=MESH)


X_LINE = [(0, i, 0, 0) for i in (1, 2, 3)]
H_LINE = [(1, 0, 0, 0)]
FIRST = [split_offset(offset) for offset in PLANE] + X_LINE + H_LINE


def kernel(
    tables_in, ids_in, lens_in, slots_in, dense_in, left_in, right_in, steps_in, out,
    tables, ids, lens, slots, dense, left_t, right_t, steps,
    table_t, pooled, send, recv, proj, shifted, total, wide,
    load_sem, table_sem, send_sem, recv_sem, x_sem, h_sem,
):
    me = place()
    h, x, z, y = me
    tab_dev, bag, samples = ids.shape
    rows = tables.shape[1]
    width = tables.shape[2]
    own = dense.shape[0]
    block = 256
    groups = recv_sem.shape[0]
    per_group = len(ORDER) // groups
    depth = per_group * tab_dev

    barrier = pltpu.get_barrier_semaphore()
    greet(me, barrier, FIRST)

    def load(source, target, sem):
        copy = pltpu.make_async_copy(source, target, sem)
        copy.start()
        return copy

    early = [load(ids_in, ids, load_sem.at[0]), load(lens_in, lens, load_sem.at[1])]
    parts = [load(tables_in.at[t], tables.at[t], table_sem.at[t]) for t in range(tab_dev)]
    late = [
        load(source, target, load_sem.at[2 + i])
        for i, (source, target) in enumerate(
            (
                (slots_in, slots),
                (dense_in, dense),
                (left_in, left_t),
                (right_in, right_t),
                (steps_in, steps),
            )
        )
    ]
    for t in range(tab_dev):
        parts[t].wait()
        table_t[t] = tables[t].T
    for copy in early:
        copy.wait()

    iota = lax.broadcasted_iota(jnp.int32, (16, block), 0).astype(jnp.int16)

    def pool_block(i, _):
        turn = lax.rem(i, 4)
        dx = lax.rem(turn * 2, 4) + turn // 2
        blk = lax.rem(h + i // 4, 2) * 4 + lax.rem(x + dx, 4)
        start = pl.multiple_of(blk * block, block)
        for t in range(tab_dev):
            length = lens[pl.ds(t, 1), pl.ds(start, block)]
            row_ids = []
            for j in range(bag):
                row = ids[t, pl.ds(j, 1), pl.ds(start, block)]
                row_ids.append(jnp.where(j < length, row, -1))
            weights = []
            for j in range(bag):
                weight = jnp.ones((1, block), jnp.float32)
                for other in range(j + 1, bag):
                    weight += (row_ids[other] == row_ids[j]).astype(jnp.float32)
                weights.append(jnp.broadcast_to(weight, (16, block)).astype(jnp.bfloat16))
            keys = [jnp.broadcast_to(row, (16, block)).astype(jnp.int16) for row in row_ids]
            result = jnp.zeros((width, block), jnp.float32)
            for chunk in range(rows // block):
                pieces = []
                for piece in range(block // 16):
                    here = iota + jnp.int16(chunk * block + piece * 16)
                    counts = jnp.zeros((16, block), jnp.bfloat16)
                    for j in reversed(range(bag)):
                        counts = jnp.where(keys[j] == here, weights[j], counts)
                    pieces.append(counts)
                result += jnp.dot(
                    table_t[t, :, pl.ds(chunk * block, block)],
                    jnp.concatenate(pieces, axis=0),
                    preferred_element_type=jnp.float32,
                )
            pooled[pl.ds(t, block, stride=tab_dev), :] = result.T
        for part in range(block // own):
            piece = pooled[pl.ds(part * own * tab_dev, own * tab_dev), :]
            send[blk * (block // own) + part] = piece.reshape(own, tab_dev, width).astype(jnp.bfloat16)
        return 0

    def post(first_step, steps_here):
        for step in range(first_step, first_step + len(steps_here)):
            to_h, to_x, to_c = partner(me, *split_offset(ORDER[step]))
            pltpu.make_async_remote_copy(
                src_ref=send.at[to_h * 64 + to_x * 16 + to_c],
                dst_ref=recv.at[:, pl.ds(step * tab_dev, tab_dev), :],
                send_sem=send_sem,
                recv_sem=recv_sem.at[step // per_group],
                device_id=(to_h, to_x, to_c),
                device_id_type=MESH,
            ).start()

    lax.fori_loop(0, 3, pool_block, 0)
    pl.semaphore_wait(barrier, len(FIRST))
    greet(me, x_sem, X_LINE)
    post(1, PLANE)
    lax.fori_loop(3, 4, pool_block, 0)
    pl.semaphore_wait(x_sem, len(X_LINE))
    greet(me, h_sem, H_LINE)
    post(16, SLAB)
    lax.fori_loop(4, samples // block, pool_block, 0)
    pl.semaphore_wait(h_sem, len(H_LINE))
    post(64, OTHER)
    recv[:, 0:tab_dev, :] = send[h * 64 + x * 16 + z * 4 + y]

    for copy in late:
        copy.wait()
    kept = left_t.shape[1]
    from_h = lax.rem(h + 2 - steps[0:1, :], 2)
    from_x = lax.rem(x + 4 - steps[1:2, :], 4)
    from_z = lax.rem(z + 4 - steps[2:3, :], 4)
    from_y = lax.rem(y + 4 - steps[3:4, :], 4)
    slot_here = (from_h * 64 + from_x * 16 + from_z * 4 + from_y) * tab_dev + steps[4:5, :]
    slot_here = slot_here.astype(jnp.float32)
    count = slots.shape[1]
    slot_col = jnp.broadcast_to(slots[...].astype(jnp.float32), (8, count)).T[:, 0:1]
    selector = jnp.where(slot_col == slot_here, 1.0, 0.0).astype(jnp.bfloat16)
    firsts = []
    for side, source in enumerate((left_t, right_t)):
        shifted[0 : count + 1, :] = source[...].astype(jnp.float32)
        firsts.append(shifted[0:8, :].T[:, 0:1])
        moved = shifted[1 : count + 1, :].T.astype(jnp.bfloat16)
        proj[pl.ds(side * kept, kept), :] = jnp.dot(
            moved, selector, preferred_element_type=jnp.float32
        ).astype(jnp.bfloat16)
    first = jnp.concatenate(firsts, axis=0)
    for b in range(own):
        row = dense[b : b + 1, :].astype(jnp.float32)
        total[b // 2, :, pl.ds(b % 2 * width, width)] = first * row

    for group in range(groups):
        arrived = per_group - (1 if group == 0 else 0)
        area = send.at[pl.ds(0, arrived)]
        pltpu.make_async_copy(area, area, recv_sem.at[group]).wait()
        last = group == groups - 1
        part = proj[:, pl.ds(group * depth, depth)]
        for pair in range(own // 2):
            both = jnp.concatenate(
                [recv[2 * pair, pl.ds(group * depth, depth), :], recv[2 * pair + 1, pl.ds(group * depth, depth), :]],
                axis=1,
            )
            mixed = total[pair] + jnp.dot(part, both, preferred_element_type=jnp.float32)
            if not last:
                total[pair] = mixed
                continue
            mixed = mixed.astype(jnp.bfloat16)
            for side in range(2):
                left = mixed[:kept, side * width : (side + 1) * width]
                right = mixed[kept:, side * width : (side + 1) * width]
                product = lax.dot_general(
                    left, right, (((1,), (1,)), ((), ())), preferred_element_type=jnp.float32
                )
                wide[pl.ds(2 * pair + side, kept, stride=own), :] = product * (1.0 / width)
    for k in range(kept):
        out[:, pl.ds(k * kept, kept)] = wide[pl.ds(k * own, own), :].astype(jnp.bfloat16)
    area = send.at[pl.ds(0, len(ORDER) - 1)]
    pltpu.make_async_copy(area, area, send_sem).wait()


def shards(tables, indices, lengths, table_slot, dense_feature, left_proj, right_proj):
    tab_dev, samples, bag = indices.shape
    width = tables.shape[2]
    rows = tables.shape[1]
    own = dense_feature.shape[0]
    kept = left_proj.shape[0]
    count = table_slot.shape[0]
    devices = len(ORDER)
    table = np.zeros((8, devices * tab_dev), np.int32)
    for step, offset in enumerate(ORDER):
        for t in range(tab_dev):
            table[:5, step * tab_dev + t] = (*split_offset(offset), t)
    vmem = pl.BlockSpec(memory_space=pltpu.VMEM)
    return pl.pallas_call(
        kernel,
        out_shape=jax.ShapeDtypeStruct((own, kept * kept), jnp.bfloat16),
        in_specs=[pl.BlockSpec(memory_space=pltpu.HBM)] * 8,
        out_specs=vmem,
        scratch_shapes=[
            pltpu.VMEM((tab_dev, rows, width), jnp.bfloat16),
            pltpu.VMEM((tab_dev, bag, samples), jnp.int32),
            pltpu.VMEM((tab_dev, samples), jnp.int32),
            pltpu.VMEM((1, count), jnp.int32),
            pltpu.VMEM((own, width), jnp.bfloat16),
            pltpu.VMEM((count + 1, kept), jnp.bfloat16),
            pltpu.VMEM((count + 1, kept), jnp.bfloat16),
            pltpu.VMEM((8, devices * tab_dev), jnp.int32),
            pltpu.VMEM((tab_dev, width, rows), jnp.bfloat16),
            pltpu.VMEM((256 * tab_dev, width), jnp.float32),
            pltpu.VMEM((devices, own, tab_dev, width), jnp.bfloat16),
            pltpu.VMEM((own, devices * tab_dev, width), jnp.bfloat16),
            pltpu.VMEM((2 * kept, devices * tab_dev), jnp.bfloat16),
            pltpu.VMEM((count + 8, kept), jnp.float32),
            pltpu.VMEM((own // 2, 2 * kept, 2 * width), jnp.float32),
            pltpu.VMEM((kept * own, kept), jnp.float32),
            pltpu.SemaphoreType.DMA((7,)),
            pltpu.SemaphoreType.DMA((tab_dev,)),
            pltpu.SemaphoreType.DMA,
            pltpu.SemaphoreType.DMA((4,)),
            pltpu.SemaphoreType.REGULAR,
            pltpu.SemaphoreType.REGULAR,
        ],
        compiler_params=pltpu.CompilerParams(
            collective_id=0, has_side_effects=True, vmem_limit_bytes=60 * 2**20
        ),
    )(
        tables,
        jnp.transpose(indices, (0, 2, 1)),
        lengths,
        table_slot.reshape(1, count),
        dense_feature,
        left_proj.T,
        right_proj.T,
        jnp.asarray(table),
    )


def solution(mesh):
    spread = P(AXES)
    return jax.shard_map(
        shards,
        mesh=mesh,
        in_specs=(spread, spread, spread, P(), spread, P(), P()),
        out_specs=spread,
        check_vma=False,
    )
```

```python
import functools

import jax
import jax.numpy as jnp
import numpy as np
from jax import lax
from jax.experimental import pallas as pl
from jax.experimental.pallas import tpu as pltpu
from jax.sharding import PartitionSpec as P

AXES = ("hst", "row", "col")
MESH = pl.DeviceIdType.MESH
LINE = (0, 1, 2, 1)


def split_offset(offset):
    return offset // 64, offset // 16 % 4, offset // 4 % 4, offset % 4


def hops(offset):
    _, dx, dz, dy = split_offset(offset)
    return LINE[dx] + LINE[dz] + LINE[dy]


def far_first(offsets):
    return sorted(offsets, key=lambda offset: -hops(offset))


PLANE = far_first(range(1, 16))
SLAB = far_first(range(32, 48)) + far_first([*range(16, 32), *range(48, 64)])
OTHER = far_first(range(64, 128))
ORDER = [0] + PLANE + SLAB + OTHER


def place():
    col = lax.axis_index("col")
    return lax.axis_index("hst"), lax.axis_index("row"), col // 4, lax.rem(col, 4)


def partner(me, dh, dx, dz, dy):
    h, x, z, y = me
    return (
        lax.rem(h + dh, 2),
        lax.rem(x + dx, 4),
        lax.rem(z + dz, 4) * 4 + lax.rem(y + dy, 4),
    )


def greet(me, sem, offsets):
    for offset in offsets:
        pl.semaphore_signal(sem, 1, device_id=partner(me, *offset), device_id_type=MESH)


X_LINE = [(0, i, 0, 0) for i in (1, 2, 3)]
H_LINE = [(1, 0, 0, 0)]
FIRST = [split_offset(offset) for offset in PLANE] + X_LINE + H_LINE


def kernel(
    tables_in, ids_in, lens_in, slots_in, dense_in, left_in, right_in, steps_in, out,
    tables, ids, lens, slots, dense, left_t, right_t, steps,
    table_t, pooled, send, recv, proj, shifted, total, wide,
    load_sem, table_sem, send_sem, recv_sem, x_sem, h_sem,
):
    me = place()
    h, x, z, y = me
    tab_dev, bag, samples = ids.shape
    rows = tables.shape[1]
    width = tables.shape[2]
    own = dense.shape[0]
    block = 256
    groups = recv_sem.shape[0]
    per_group = len(ORDER) // groups
    depth = per_group * tab_dev

    barrier = pltpu.get_barrier_semaphore()
    greet(me, barrier, FIRST)

    def load(source, target, sem):
        copy = pltpu.make_async_copy(source, target, sem)
        copy.start()
        return copy

    early = [load(ids_in, ids, load_sem.at[0]), load(lens_in, lens, load_sem.at[1])]
    parts = [load(tables_in.at[t], tables.at[t], table_sem.at[t]) for t in range(tab_dev)]
    late = [
        load(source, target, load_sem.at[2 + i])
        for i, (source, target) in enumerate(
            (
                (slots_in, slots),
                (dense_in, dense),
                (left_in, left_t),
                (right_in, right_t),
                (steps_in, steps),
            )
        )
    ]
    for copy in early:
        copy.wait()

    iota = lax.broadcasted_iota(jnp.int32, (16, block), 0).astype(jnp.int16)

    def pool_block(i, _, first=False):
        turn = lax.rem(i, 4)
        dx = lax.rem(turn * 2, 4) + turn // 2
        blk = lax.rem(h + i // 4, 2) * 4 + lax.rem(x + dx, 4)
        start = pl.multiple_of(blk * block, block)
        for t in range(tab_dev):
            if first:
                parts[t].wait()
                table_t[t] = tables[t].T
            length = lens[pl.ds(t, 1), pl.ds(start, block)]
            row_ids = []
            for j in range(bag):
                row = ids[t, pl.ds(j, 1), pl.ds(start, block)]
                row_ids.append(jnp.where(j < length, row, -1))
            weights = []
            for j in range(bag):
                weight = jnp.ones((1, block), jnp.float32)
                for other in range(j + 1, bag):
                    weight += (row_ids[other] == row_ids[j]).astype(jnp.float32)
                weights.append(jnp.broadcast_to(weight, (16, block)).astype(jnp.bfloat16))
            keys = [jnp.broadcast_to(row, (16, block)).astype(jnp.int16) for row in row_ids]
            result = jnp.zeros((width, block), jnp.float32)
            for chunk in range(rows // block):
                pieces = []
                for piece in range(block // 16):
                    here = iota + jnp.int16(chunk * block + piece * 16)
                    counts = jnp.zeros((16, block), jnp.bfloat16)
                    for j in reversed(range(bag)):
                        counts = jnp.where(keys[j] == here, weights[j], counts)
                    pieces.append(counts)
                result += jnp.dot(
                    table_t[t, :, pl.ds(chunk * block, block)],
                    jnp.concatenate(pieces, axis=0),
                    preferred_element_type=jnp.float32,
                )
            pooled[pl.ds(t, block, stride=tab_dev), :] = result.T
        for part in range(block // own):
            piece = pooled[pl.ds(part * own * tab_dev, own * tab_dev), :]
            send[blk * (block // own) + part] = piece.reshape(own, tab_dev, width).astype(jnp.bfloat16)
        return 0

    def post(first_step, steps_here):
        for step in range(first_step, first_step + len(steps_here)):
            to_h, to_x, to_c = partner(me, *split_offset(ORDER[step]))
            pltpu.make_async_remote_copy(
                src_ref=send.at[to_h * 64 + to_x * 16 + to_c],
                dst_ref=recv.at[:, pl.ds(step * tab_dev, tab_dev), :],
                send_sem=send_sem,
                recv_sem=recv_sem.at[step // per_group],
                device_id=(to_h, to_x, to_c),
                device_id_type=MESH,
            ).start()

    pool_block(0, 0, first=True)
    pl.semaphore_wait(barrier, len(FIRST))
    greet(me, x_sem, X_LINE)
    post(1, PLANE)
    lax.fori_loop(1, 2, pool_block, 0)
    pl.semaphore_wait(x_sem, len(X_LINE))
    greet(me, h_sem, H_LINE)
    post(16, SLAB[:16])
    lax.fori_loop(2, 4, pool_block, 0)
    post(32, SLAB[16:])
    lax.fori_loop(4, 8, pool_block, 0)
    pl.semaphore_wait(h_sem, len(H_LINE))
    post(64, OTHER)
    recv[:, 0:tab_dev, :] = send[h * 64 + x * 16 + z * 4 + y]

    for copy in late:
        copy.wait()
    kept = left_t.shape[1]
    from_h = lax.rem(h + 2 - steps[0:1, :], 2)
    from_x = lax.rem(x + 4 - steps[1:2, :], 4)
    from_z = lax.rem(z + 4 - steps[2:3, :], 4)
    from_y = lax.rem(y + 4 - steps[3:4, :], 4)
    slot_here = (from_h * 64 + from_x * 16 + from_z * 4 + from_y) * tab_dev + steps[4:5, :]
    slot_here = slot_here.astype(jnp.float32)
    count = slots.shape[1]
    slot_col = jnp.broadcast_to(slots[...].astype(jnp.float32), (8, count)).T[:, 0:1]
    selector = jnp.where(slot_col == slot_here, 1.0, 0.0).astype(jnp.bfloat16)
    firsts = []
    for side, source in enumerate((left_t, right_t)):
        shifted[0 : count + 1, :] = source[...].astype(jnp.float32)
        firsts.append(shifted[0:8, :].T[:, 0:1])
        moved = shifted[1 : count + 1, :].T.astype(jnp.bfloat16)
        proj[pl.ds(side * kept, kept), :] = jnp.dot(
            moved, selector, preferred_element_type=jnp.float32
        ).astype(jnp.bfloat16)
    first = jnp.concatenate(firsts, axis=0)
    for b in range(own):
        row = dense[b : b + 1, :].astype(jnp.float32)
        total[b // 2, :, pl.ds(b % 2 * width, width)] = first * row

    for group in range(groups):
        arrived = per_group - (1 if group == 0 else 0)
        area = send.at[pl.ds(0, arrived)]
        pltpu.make_async_copy(area, area, recv_sem.at[group]).wait()
        last = group == groups - 1
        part = proj[:, pl.ds(group * depth, depth)]
        for pair in range(own // 2):
            both = jnp.concatenate(
                [recv[2 * pair, pl.ds(group * depth, depth), :], recv[2 * pair + 1, pl.ds(group * depth, depth), :]],
                axis=1,
            )
            mixed = total[pair] + jnp.dot(part, both, preferred_element_type=jnp.float32)
            if not last:
                total[pair] = mixed
                continue
            mixed = mixed.astype(jnp.bfloat16)
            for side in range(2):
                left = mixed[:kept, side * width : (side + 1) * width]
                right = mixed[kept:, side * width : (side + 1) * width]
                product = lax.dot_general(
                    left, right, (((1,), (1,)), ((), ())), preferred_element_type=jnp.float32
                )
                wide[pl.ds(2 * pair + side, kept, stride=own), :] = product * (1.0 / width)
    for k in range(kept):
        out[:, pl.ds(k * kept, kept)] = wide[pl.ds(k * own, own), :].astype(jnp.bfloat16)
    area = send.at[pl.ds(0, len(ORDER) - 1)]
    pltpu.make_async_copy(area, area, send_sem).wait()


def shards(tables, indices, lengths, table_slot, dense_feature, left_proj, right_proj):
    tab_dev, samples, bag = indices.shape
    width = tables.shape[2]
    rows = tables.shape[1]
    own = dense_feature.shape[0]
    kept = left_proj.shape[0]
    count = table_slot.shape[0]
    devices = len(ORDER)
    table = np.zeros((8, devices * tab_dev), np.int32)
    for step, offset in enumerate(ORDER):
        for t in range(tab_dev):
            table[:5, step * tab_dev + t] = (*split_offset(offset), t)
    vmem = pl.BlockSpec(memory_space=pltpu.VMEM)
    return pl.pallas_call(
        kernel,
        out_shape=jax.ShapeDtypeStruct((own, kept * kept), jnp.bfloat16),
        in_specs=[pl.BlockSpec(memory_space=pltpu.HBM)] * 8,
        out_specs=vmem,
        scratch_shapes=[
            pltpu.VMEM((tab_dev, rows, width), jnp.bfloat16),
            pltpu.VMEM((tab_dev, bag, samples), jnp.int32),
            pltpu.VMEM((tab_dev, samples), jnp.int32),
            pltpu.VMEM((1, count), jnp.int32),
            pltpu.VMEM((own, width), jnp.bfloat16),
            pltpu.VMEM((count + 1, kept), jnp.bfloat16),
            pltpu.VMEM((count + 1, kept), jnp.bfloat16),
            pltpu.VMEM((8, devices * tab_dev), jnp.int32),
            pltpu.VMEM((tab_dev, width, rows), jnp.bfloat16),
            pltpu.VMEM((256 * tab_dev, width), jnp.float32),
            pltpu.VMEM((devices, own, tab_dev, width), jnp.bfloat16),
            pltpu.VMEM((own, devices * tab_dev, width), jnp.bfloat16),
            pltpu.VMEM((2 * kept, devices * tab_dev), jnp.bfloat16),
            pltpu.VMEM((count + 8, kept), jnp.float32),
            pltpu.VMEM((own // 2, 2 * kept, 2 * width), jnp.float32),
            pltpu.VMEM((kept * own, kept), jnp.float32),
            pltpu.SemaphoreType.DMA((7,)),
            pltpu.SemaphoreType.DMA((tab_dev,)),
            pltpu.SemaphoreType.DMA,
            pltpu.SemaphoreType.DMA((4,)),
            pltpu.SemaphoreType.REGULAR,
            pltpu.SemaphoreType.REGULAR,
        ],
        compiler_params=pltpu.CompilerParams(
            collective_id=0, has_side_effects=True, vmem_limit_bytes=60 * 2**20
        ),
    )(
        tables,
        jnp.transpose(indices, (0, 2, 1)),
        lengths,
        table_slot.reshape(1, count),
        dense_feature,
        left_proj.T,
        right_proj.T,
        jnp.asarray(table),
    )


def solution(mesh):
    spread = P(AXES)
    return jax.shard_map(
        shards,
        mesh=mesh,
        in_specs=(spread, spread, spread, P(), spread, P(), P()),
        out_specs=spread,
        check_vma=False,
    )
```

```python
import functools

import jax
import jax.numpy as jnp
import numpy as np
from jax import lax
from jax.experimental import pallas as pl
from jax.experimental.pallas import tpu as pltpu
from jax.sharding import PartitionSpec as P

AXES = ("hst", "row", "col")
MESH = pl.DeviceIdType.MESH


def split_offset(offset):
    return offset // 64, offset // 16 % 4, offset // 4 % 4, offset % 4


PLANE = [10, 6, 9, 11, 14, 2, 5, 7, 8, 13, 15, 1, 3, 4, 12]
SLAB = [42, 38, 41, 43, 46, 34, 37, 39, 40, 45, 47, 33, 35, 36, 44, 32, 26, 58, 22, 54, 25, 57, 27, 59, 30, 62, 18, 50, 21, 53, 23, 55, 24, 56, 29, 61, 31, 63, 17, 49, 19, 51, 20, 52, 28, 60, 16, 48]
OTHER = [106, 102, 105, 90, 122, 107, 110, 98, 101, 86, 118, 103, 104, 89, 121, 74, 91, 123, 109, 85, 126, 111, 97, 82, 114, 99, 100, 94, 117, 70, 87, 119, 88, 120, 73, 75, 108, 93, 125, 78, 95, 127, 96, 81, 113, 66, 83, 115, 84, 116, 69, 71, 72, 92, 124, 77, 79, 80, 112, 65, 67, 68, 76, 64]
ORDER = [0] + PLANE + SLAB + OTHER


def place():
    col = lax.axis_index("col")
    return lax.axis_index("hst"), lax.axis_index("row"), col // 4, lax.rem(col, 4)


def partner(me, dh, dx, dz, dy):
    h, x, z, y = me
    return (
        lax.rem(h + dh, 2),
        lax.rem(x + dx, 4),
        lax.rem(z + dz, 4) * 4 + lax.rem(y + dy, 4),
    )


def greet(me, sem, offsets):
    for offset in offsets:
        pl.semaphore_signal(sem, 1, device_id=partner(me, *offset), device_id_type=MESH)


X_LINE = [(0, i, 0, 0) for i in (1, 2, 3)]
H_LINE = [(1, 0, 0, 0)]
FIRST = [split_offset(offset) for offset in PLANE] + X_LINE + H_LINE


def kernel(
    tables_in, ids_in, lens_in, slots_in, dense_in, left_in, right_in, steps_in, out,
    tables, ids, lens, slots, dense, left_t, right_t, steps,
    table_t, pooled, send, recv, proj, shifted, total, wide,
    load_sem, table_sem, send_sem, recv_sem, x_sem, h_sem,
):
    me = place()
    h, x, z, y = me
    tab_dev, bag, samples = ids.shape
    rows = tables.shape[1]
    width = tables.shape[2]
    own = dense.shape[0]
    block = 256
    groups = recv_sem.shape[0]
    per_group = len(ORDER) // groups
    depth = per_group * tab_dev

    barrier = pltpu.get_barrier_semaphore()
    greet(me, barrier, FIRST)

    def load(source, target, sem):
        copy = pltpu.make_async_copy(source, target, sem)
        copy.start()
        return copy

    early = [load(ids_in, ids, load_sem.at[0]), load(lens_in, lens, load_sem.at[1])]
    parts = [load(tables_in.at[t], tables.at[t], table_sem.at[t]) for t in range(tab_dev)]
    late = [
        load(source, target, load_sem.at[2 + i])
        for i, (source, target) in enumerate(
            (
                (slots_in, slots),
                (dense_in, dense),
                (left_in, left_t),
                (right_in, right_t),
                (steps_in, steps),
            )
        )
    ]
    for copy in early:
        copy.wait()

    iota = lax.broadcasted_iota(jnp.int32, (16, block), 0).astype(jnp.int16)

    def pool_block(i, _, first=False):
        turn = lax.rem(i, 4)
        dx = lax.rem(turn * 2, 4) + turn // 2
        blk = lax.rem(h + i // 4, 2) * 4 + lax.rem(x + dx, 4)
        start = pl.multiple_of(blk * block, block)
        for t in range(tab_dev):
            if first:
                parts[t].wait()
                table_t[t] = tables[t].T
            length = lens[pl.ds(t, 1), pl.ds(start, block)]
            row_ids = []
            for j in range(bag):
                row = ids[t, pl.ds(j, 1), pl.ds(start, block)]
                row_ids.append(jnp.where(j < length, row, -1))
            weights = []
            for j in range(bag):
                weight = jnp.ones((1, block), jnp.float32)
                for other in range(j + 1, bag):
                    weight += (row_ids[other] == row_ids[j]).astype(jnp.float32)
                weights.append(jnp.broadcast_to(weight, (16, block)).astype(jnp.bfloat16))
            keys = [jnp.broadcast_to(row, (16, block)).astype(jnp.int16) for row in row_ids]
            result = jnp.zeros((width, block), jnp.float32)
            for chunk in range(rows // block):
                pieces = []
                for piece in range(block // 16):
                    here = iota + jnp.int16(chunk * block + piece * 16)
                    counts = jnp.zeros((16, block), jnp.bfloat16)
                    for j in reversed(range(bag)):
                        counts = jnp.where(keys[j] == here, weights[j], counts)
                    pieces.append(counts)
                result += jnp.dot(
                    table_t[t, :, pl.ds(chunk * block, block)],
                    jnp.concatenate(pieces, axis=0),
                    preferred_element_type=jnp.float32,
                )
            pooled[pl.ds(t, block, stride=tab_dev), :] = result.T
        for part in range(block // own):
            piece = pooled[pl.ds(part * own * tab_dev, own * tab_dev), :]
            send[blk * (block // own) + part] = piece.reshape(own, tab_dev, width).astype(jnp.bfloat16)
        return 0

    def post(first_step, steps_here):
        for step in range(first_step, first_step + len(steps_here)):
            to_h, to_x, to_c = partner(me, *split_offset(ORDER[step]))
            pltpu.make_async_remote_copy(
                src_ref=send.at[to_h * 64 + to_x * 16 + to_c],
                dst_ref=recv.at[:, pl.ds(step * tab_dev, tab_dev), :],
                send_sem=send_sem,
                recv_sem=recv_sem.at[step // per_group],
                device_id=(to_h, to_x, to_c),
                device_id_type=MESH,
            ).start()

    pool_block(0, 0, first=True)
    pl.semaphore_wait(barrier, len(FIRST))
    greet(me, x_sem, X_LINE)
    post(1, PLANE)
    lax.fori_loop(1, 2, pool_block, 0)
    pl.semaphore_wait(x_sem, len(X_LINE))
    greet(me, h_sem, H_LINE)
    post(16, SLAB[:16])
    lax.fori_loop(2, 4, pool_block, 0)
    post(32, SLAB[16:])
    lax.fori_loop(4, 8, pool_block, 0)
    pl.semaphore_wait(h_sem, len(H_LINE))
    post(64, OTHER)
    recv[:, 0:tab_dev, :] = send[h * 64 + x * 16 + z * 4 + y]

    for copy in late:
        copy.wait()
    kept = left_t.shape[1]
    from_h = lax.rem(h + 2 - steps[0:1, :], 2)
    from_x = lax.rem(x + 4 - steps[1:2, :], 4)
    from_z = lax.rem(z + 4 - steps[2:3, :], 4)
    from_y = lax.rem(y + 4 - steps[3:4, :], 4)
    slot_here = (from_h * 64 + from_x * 16 + from_z * 4 + from_y) * tab_dev + steps[4:5, :]
    slot_here = slot_here.astype(jnp.float32)
    count = slots.shape[1]
    slot_col = jnp.broadcast_to(slots[...].astype(jnp.float32), (8, count)).T[:, 0:1]
    selector = jnp.where(slot_col == slot_here, 1.0, 0.0).astype(jnp.bfloat16)
    firsts = []
    for side, source in enumerate((left_t, right_t)):
        shifted[0 : count + 1, :] = source[...].astype(jnp.float32)
        firsts.append(shifted[0:8, :].T[:, 0:1])
        moved = shifted[1 : count + 1, :].T.astype(jnp.bfloat16)
        proj[pl.ds(side * kept, kept), :] = jnp.dot(
            moved, selector, preferred_element_type=jnp.float32
        ).astype(jnp.bfloat16)
    first = jnp.concatenate(firsts, axis=0)
    for b in range(own):
        row = dense[b : b + 1, :].astype(jnp.float32)
        total[b // 2, :, pl.ds(b % 2 * width, width)] = first * row

    for group in range(groups):
        arrived = per_group - (1 if group == 0 else 0)
        area = send.at[pl.ds(0, arrived)]
        pltpu.make_async_copy(area, area, recv_sem.at[group]).wait()
        last = group == groups - 1
        part = proj[:, pl.ds(group * depth, depth)]
        for pair in range(own // 2):
            both = jnp.concatenate(
                [recv[2 * pair, pl.ds(group * depth, depth), :], recv[2 * pair + 1, pl.ds(group * depth, depth), :]],
                axis=1,
            )
            mixed = total[pair] + jnp.dot(part, both, preferred_element_type=jnp.float32)
            if not last:
                total[pair] = mixed
                continue
            mixed = mixed.astype(jnp.bfloat16)
            for side in range(2):
                left = mixed[:kept, side * width : (side + 1) * width]
                right = mixed[kept:, side * width : (side + 1) * width]
                product = lax.dot_general(
                    left, right, (((1,), (1,)), ((), ())), preferred_element_type=jnp.float32
                )
                wide[pl.ds(2 * pair + side, kept, stride=own), :] = product * (1.0 / width)
    for k in range(kept):
        out[:, pl.ds(k * kept, kept)] = wide[pl.ds(k * own, own), :].astype(jnp.bfloat16)
    area = send.at[pl.ds(0, len(ORDER) - 1)]
    pltpu.make_async_copy(area, area, send_sem).wait()


def shards(tables, indices, lengths, table_slot, dense_feature, left_proj, right_proj):
    tab_dev, samples, bag = indices.shape
    width = tables.shape[2]
    rows = tables.shape[1]
    own = dense_feature.shape[0]
    kept = left_proj.shape[0]
    count = table_slot.shape[0]
    devices = len(ORDER)
    table = np.zeros((8, devices * tab_dev), np.int32)
    for step, offset in enumerate(ORDER):
        for t in range(tab_dev):
            table[:5, step * tab_dev + t] = (*split_offset(offset), t)
    vmem = pl.BlockSpec(memory_space=pltpu.VMEM)
    return pl.pallas_call(
        kernel,
        out_shape=jax.ShapeDtypeStruct((own, kept * kept), jnp.bfloat16),
        in_specs=[pl.BlockSpec(memory_space=pltpu.HBM)] * 8,
        out_specs=vmem,
        scratch_shapes=[
            pltpu.VMEM((tab_dev, rows, width), jnp.bfloat16),
            pltpu.VMEM((tab_dev, bag, samples), jnp.int32),
            pltpu.VMEM((tab_dev, samples), jnp.int32),
            pltpu.VMEM((1, count), jnp.int32),
            pltpu.VMEM((own, width), jnp.bfloat16),
            pltpu.VMEM((count + 1, kept), jnp.bfloat16),
            pltpu.VMEM((count + 1, kept), jnp.bfloat16),
            pltpu.VMEM((8, devices * tab_dev), jnp.int32),
            pltpu.VMEM((tab_dev, width, rows), jnp.bfloat16),
            pltpu.VMEM((256 * tab_dev, width), jnp.float32),
            pltpu.VMEM((devices, own, tab_dev, width), jnp.bfloat16),
            pltpu.VMEM((own, devices * tab_dev, width), jnp.bfloat16),
            pltpu.VMEM((2 * kept, devices * tab_dev), jnp.bfloat16),
            pltpu.VMEM((count + 8, kept), jnp.float32),
            pltpu.VMEM((own // 2, 2 * kept, 2 * width), jnp.float32),
            pltpu.VMEM((kept * own, kept), jnp.float32),
            pltpu.SemaphoreType.DMA((7,)),
            pltpu.SemaphoreType.DMA((tab_dev,)),
            pltpu.SemaphoreType.DMA,
            pltpu.SemaphoreType.DMA((4,)),
            pltpu.SemaphoreType.REGULAR,
            pltpu.SemaphoreType.REGULAR,
        ],
        compiler_params=pltpu.CompilerParams(
            collective_id=0, has_side_effects=True, vmem_limit_bytes=60 * 2**20
        ),
    )(
        tables,
        jnp.transpose(indices, (0, 2, 1)),
        lengths,
        table_slot.reshape(1, count),
        dense_feature,
        left_proj.T,
        right_proj.T,
        jnp.asarray(table),
    )


def solution(mesh):
    spread = P(AXES)
    return jax.shard_map(
        shards,
        mesh=mesh,
        in_specs=(spread, spread, spread, P(), spread, P(), P()),
        out_specs=spread,
        check_vma=False,
    )
```

```python
import functools

import jax
import jax.numpy as jnp
import numpy as np
from jax import lax
from jax.experimental import pallas as pl
from jax.experimental.pallas import tpu as pltpu
from jax.sharding import PartitionSpec as P

AXES = ("hst", "row", "col")
MESH = pl.DeviceIdType.MESH


def split_offset(offset):
    return offset // 64, offset // 16 % 4, offset // 4 % 4, offset % 4


PLANE = [10, 6, 9, 11, 14, 2, 5, 7, 8, 13, 15, 1, 3, 4, 12]
SLAB = [42, 38, 41, 43, 46, 34, 37, 39, 40, 45, 47, 33, 35, 36, 44, 32, 26, 58, 22, 54, 25, 57, 27, 59, 30, 62, 18, 50, 21, 53, 23, 55, 24, 56, 29, 61, 31, 63, 17, 49, 19, 51, 20, 52, 28, 60, 16, 48]
OTHER = [106, 102, 105, 90, 122, 107, 110, 98, 101, 86, 118, 103, 104, 89, 121, 74, 91, 123, 109, 85, 126, 111, 97, 82, 114, 99, 100, 94, 117, 70, 87, 119, 88, 120, 73, 75, 108, 93, 125, 78, 95, 127, 96, 81, 113, 66, 83, 115, 84, 116, 69, 71, 72, 92, 124, 77, 79, 80, 112, 65, 67, 68, 76, 64]
ORDER = [0] + PLANE + SLAB + OTHER


def place():
    col = lax.axis_index("col")
    return lax.axis_index("hst"), lax.axis_index("row"), col // 4, lax.rem(col, 4)


def partner(me, dh, dx, dz, dy):
    h, x, z, y = me
    return (
        lax.rem(h + dh, 2),
        lax.rem(x + dx, 4),
        lax.rem(z + dz, 4) * 4 + lax.rem(y + dy, 4),
    )


def greet(me, sem, offsets):
    for offset in offsets:
        pl.semaphore_signal(sem, 1, device_id=partner(me, *offset), device_id_type=MESH)


X_LINE = [(0, i, 0, 0) for i in (1, 2, 3)]
H_LINE = [(1, 0, 0, 0)]
FIRST = [split_offset(offset) for offset in PLANE] + X_LINE + H_LINE


def kernel(
    tables_in, ids_in, lens_in, slots_in, dense_in, left_in, right_in, steps_in, out,
    tables, ids, lens, slots, dense, left_t, right_t, steps,
    table_t, pooled, send, recv, proj, shifted, total, wide, flat,
    out_sem, load_sem, table_sem, send_sem, recv_sem, x_sem, h_sem,
):
    me = place()
    h, x, z, y = me
    tab_dev, bag, samples = ids.shape
    rows = tables.shape[1]
    width = tables.shape[2]
    own = dense.shape[0]
    block = 256
    groups = recv_sem.shape[0]
    per_group = len(ORDER) // groups
    depth = per_group * tab_dev

    barrier = pltpu.get_barrier_semaphore()
    greet(me, barrier, FIRST)

    def load(source, target, sem):
        copy = pltpu.make_async_copy(source, target, sem)
        copy.start()
        return copy

    early = [load(ids_in, ids, load_sem.at[0]), load(lens_in, lens, load_sem.at[1])]
    parts = [load(tables_in.at[t], tables.at[t], table_sem.at[t]) for t in range(tab_dev)]
    late = [
        load(source, target, load_sem.at[2 + i])
        for i, (source, target) in enumerate(
            (
                (slots_in, slots),
                (dense_in, dense),
                (left_in, left_t),
                (right_in, right_t),
                (steps_in, steps),
            )
        )
    ]
    for copy in early:
        copy.wait()

    iota = lax.broadcasted_iota(jnp.int32, (16, block), 0).astype(jnp.int16)

    def pool_block(i, _, first=False):
        turn = lax.rem(i, 4)
        dx = lax.rem(turn * 2, 4) + turn // 2
        blk = lax.rem(h + i // 4, 2) * 4 + lax.rem(x + dx, 4)
        start = pl.multiple_of(blk * block, block)
        for t in range(tab_dev):
            if first:
                parts[t].wait()
                table_t[t] = tables[t].T
            length = lens[pl.ds(t, 1), pl.ds(start, block)]
            row_ids = []
            for j in range(bag):
                row = ids[t, pl.ds(j, 1), pl.ds(start, block)]
                row_ids.append(jnp.where(j < length, row, -1))
            weights = []
            for j in range(bag):
                weight = jnp.ones((1, block), jnp.float32)
                for other in range(j + 1, bag):
                    weight += (row_ids[other] == row_ids[j]).astype(jnp.float32)
                weights.append(jnp.broadcast_to(weight, (16, block)).astype(jnp.bfloat16))
            keys = [jnp.broadcast_to(row, (16, block)).astype(jnp.int16) for row in row_ids]
            result = jnp.zeros((width, block), jnp.float32)
            for chunk in range(rows // block):
                pieces = []
                for piece in range(block // 16):
                    here = iota + jnp.int16(chunk * block + piece * 16)
                    counts = jnp.zeros((16, block), jnp.bfloat16)
                    for j in reversed(range(bag)):
                        counts = jnp.where(keys[j] == here, weights[j], counts)
                    pieces.append(counts)
                result += jnp.dot(
                    table_t[t, :, pl.ds(chunk * block, block)],
                    jnp.concatenate(pieces, axis=0),
                    preferred_element_type=jnp.float32,
                )
            pooled[pl.ds(t, block, stride=tab_dev), :] = result.T
        for part in range(block // own):
            piece = pooled[pl.ds(part * own * tab_dev, own * tab_dev), :]
            send[blk * (block // own) + part] = piece.reshape(own, tab_dev, width).astype(jnp.bfloat16)
        return 0

    def post(first_step, steps_here):
        for step in range(first_step, first_step + len(steps_here)):
            to_h, to_x, to_c = partner(me, *split_offset(ORDER[step]))
            pltpu.make_async_remote_copy(
                src_ref=send.at[to_h * 64 + to_x * 16 + to_c],
                dst_ref=recv.at[:, pl.ds(step * tab_dev, tab_dev), :],
                send_sem=send_sem,
                recv_sem=recv_sem.at[step // per_group],
                device_id=(to_h, to_x, to_c),
                device_id_type=MESH,
            ).start()

    pool_block(0, 0, first=True)
    pl.semaphore_wait(barrier, len(FIRST))
    greet(me, x_sem, X_LINE)
    post(1, PLANE)
    lax.fori_loop(1, 2, pool_block, 0)
    pl.semaphore_wait(x_sem, len(X_LINE))
    greet(me, h_sem, H_LINE)
    post(16, SLAB[:16])
    lax.fori_loop(2, 4, pool_block, 0)
    post(32, SLAB[16:])
    lax.fori_loop(4, 8, pool_block, 0)
    pl.semaphore_wait(h_sem, len(H_LINE))
    post(64, OTHER)
    recv[:, 0:tab_dev, :] = send[h * 64 + x * 16 + z * 4 + y]

    for copy in late:
        copy.wait()
    kept = left_t.shape[1]
    from_h = lax.rem(h + 2 - steps[0:1, :], 2)
    from_x = lax.rem(x + 4 - steps[1:2, :], 4)
    from_z = lax.rem(z + 4 - steps[2:3, :], 4)
    from_y = lax.rem(y + 4 - steps[3:4, :], 4)
    slot_here = (from_h * 64 + from_x * 16 + from_z * 4 + from_y) * tab_dev + steps[4:5, :]
    slot_here = slot_here.astype(jnp.float32)
    count = slots.shape[1]
    slot_col = jnp.broadcast_to(slots[...].astype(jnp.float32), (8, count)).T[:, 0:1]
    selector = jnp.where(slot_col == slot_here, 1.0, 0.0).astype(jnp.bfloat16)
    firsts = []
    for side, source in enumerate((left_t, right_t)):
        shifted[0 : count + 1, :] = source[...].astype(jnp.float32)
        firsts.append(shifted[0:8, :].T[:, 0:1])
        moved = shifted[1 : count + 1, :].T.astype(jnp.bfloat16)
        proj[pl.ds(side * kept, kept), :] = jnp.dot(
            moved, selector, preferred_element_type=jnp.float32
        ).astype(jnp.bfloat16)
    first = jnp.concatenate(firsts, axis=0)
    for b in range(own):
        row = dense[b : b + 1, :].astype(jnp.float32)
        total[b // 2, :, pl.ds(b % 2 * width, width)] = first * row

    stores = []
    for group in range(groups):
        arrived = per_group - (1 if group == 0 else 0)
        area = send.at[pl.ds(0, arrived)]
        pltpu.make_async_copy(area, area, recv_sem.at[group]).wait()
        last = group == groups - 1
        part = proj[:, pl.ds(group * depth, depth)]
        for pair in range(own // 2):
            both = jnp.concatenate(
                [recv[2 * pair, pl.ds(group * depth, depth), :], recv[2 * pair + 1, pl.ds(group * depth, depth), :]],
                axis=1,
            )
            mixed = total[pair] + jnp.dot(part, both, preferred_element_type=jnp.float32)
            if not last:
                total[pair] = mixed
                continue
            mixed = mixed.astype(jnp.bfloat16)
            for side in range(2):
                left = mixed[:kept, side * width : (side + 1) * width]
                right = mixed[kept:, side * width : (side + 1) * width]
                product = lax.dot_general(
                    left, right, (((1,), (1,)), ((), ())), preferred_element_type=jnp.float32
                )
                wide[pl.ds(2 * pair + side, kept, stride=own), :] = product * (1.0 / width)
            if (2 * pair + 2) % 8 == 0:
                low = 2 * pair - 6
                for k in range(kept):
                    flat[low // 8, :, pl.ds(k * kept, kept)] = wide[
                        pl.ds(k * own + low, 8), :
                    ].astype(jnp.bfloat16)
                stores.append(load(flat.at[low // 8], out.at[pl.ds(low, 8), :], out_sem.at[low // 8]))
    area = send.at[pl.ds(0, len(ORDER) - 1)]
    pltpu.make_async_copy(area, area, send_sem).wait()
    for copy in stores:
        copy.wait()


def shards(tables, indices, lengths, table_slot, dense_feature, left_proj, right_proj):
    tab_dev, samples, bag = indices.shape
    width = tables.shape[2]
    rows = tables.shape[1]
    own = dense_feature.shape[0]
    kept = left_proj.shape[0]
    count = table_slot.shape[0]
    devices = len(ORDER)
    table = np.zeros((8, devices * tab_dev), np.int32)
    for step, offset in enumerate(ORDER):
        for t in range(tab_dev):
            table[:5, step * tab_dev + t] = (*split_offset(offset), t)
    return pl.pallas_call(
        kernel,
        out_shape=jax.ShapeDtypeStruct((own, kept * kept), jnp.bfloat16),
        in_specs=[pl.BlockSpec(memory_space=pltpu.HBM)] * 8,
        out_specs=pl.BlockSpec(memory_space=pltpu.HBM),
        scratch_shapes=[
            pltpu.VMEM((tab_dev, rows, width), jnp.bfloat16),
            pltpu.VMEM((tab_dev, bag, samples), jnp.int32),
            pltpu.VMEM((tab_dev, samples), jnp.int32),
            pltpu.VMEM((1, count), jnp.int32),
            pltpu.VMEM((own, width), jnp.bfloat16),
            pltpu.VMEM((count + 1, kept), jnp.bfloat16),
            pltpu.VMEM((count + 1, kept), jnp.bfloat16),
            pltpu.VMEM((8, devices * tab_dev), jnp.int32),
            pltpu.VMEM((tab_dev, width, rows), jnp.bfloat16),
            pltpu.VMEM((256 * tab_dev, width), jnp.float32),
            pltpu.VMEM((devices, own, tab_dev, width), jnp.bfloat16),
            pltpu.VMEM((own, devices * tab_dev, width), jnp.bfloat16),
            pltpu.VMEM((2 * kept, devices * tab_dev), jnp.bfloat16),
            pltpu.VMEM((count + 8, kept), jnp.float32),
            pltpu.VMEM((own // 2, 2 * kept, 2 * width), jnp.float32),
            pltpu.VMEM((kept * own, kept), jnp.float32),
            pltpu.VMEM((own // 8, 8, kept * kept), jnp.bfloat16),
            pltpu.SemaphoreType.DMA((own // 8,)),
            pltpu.SemaphoreType.DMA((7,)),
            pltpu.SemaphoreType.DMA((tab_dev,)),
            pltpu.SemaphoreType.DMA,
            pltpu.SemaphoreType.DMA((4,)),
            pltpu.SemaphoreType.REGULAR,
            pltpu.SemaphoreType.REGULAR,
        ],
        compiler_params=pltpu.CompilerParams(
            collective_id=0, has_side_effects=True, vmem_limit_bytes=60 * 2**20
        ),
    )(
        tables,
        jnp.transpose(indices, (0, 2, 1)),
        lengths,
        table_slot.reshape(1, count),
        dense_feature,
        left_proj.T,
        right_proj.T,
        jnp.asarray(table),
    )


def solution(mesh):
    spread = P(AXES)
    return jax.shard_map(
        shards,
        mesh=mesh,
        in_specs=(spread, spread, spread, P(), spread, P(), P()),
        out_specs=spread,
        check_vma=False,
    )
```
